32 devices in a mesh: gx: 4 (over y, x), gy: 4 (over z), gz: 2 (over core).
Axes of the slice: x: 2, y: 2, z: 4, core: 2. Of those that a mesh axis runs over, the one named last changes fastest.
Arguments:
- correlators: bfloat16 [32, 32, 32, 16, 128], P(None, 'gx', 'gy', 'gz'), may hold values from -6 to 6
- momenta: int32 [125, 3], replicated, may hold values from -8 to 7
- source_channel: int32 [64], replicated, may hold values from 0 to 63
- phase_code: int32 [64], replicated, may hold values from 0 to 3
Outputs:
- projected: float32 [32, 125, 128], P('gx', None, ('gy', 'gz'))
The draws below stay inside these ranges and needn't reach their ends.
All inputs are finite; a program needn't handle non-finite values.
Results may differ from the reference program's by a relative error of at most 0.002.
Values sent between devices are 32-bit elements; how exact they have to be, the bound alone decides.
A program may use at most 64 MiB of HBM per device.

```python
import math
import jax
import jax.numpy as jnp
from jax import lax

CH = 64
MOM = 125
TW = 32
NX = 32
NY = 32
NZ = 16


def set_ends(drawn, key, least, top_value):
    index_at = [jax.random.randint(jax.random.fold_in(key, axis), (), 0, length) for axis, length in enumerate(drawn.shape)]
    main_axis = drawn.shape.index(max(drawn.shape))
    beside = index_at[:main_axis] + [(index_at[main_axis] + 1) % drawn.shape[main_axis]] + index_at[main_axis + 1:]
    return drawn.at[tuple(index_at)].set(least).at[tuple(beside)].set(top_value)


def shard_levels(own_key, shape, shards, low, top_value):
    loudness, own = 1.0, jax.random.fold_in(own_key, 6)
    for dim, blocks in shards:
        steps = jnp.exp(jax.random.uniform(jax.random.fold_in(own, dim), (blocks,), jnp.float32, low / len(shards), top_value / len(shards)))
        loudness = loudness * jnp.repeat(steps, shape[dim] // blocks).reshape([-1 if axis == dim else 1 for axis in range(len(shape))])
    return loudness


def normal_values(own_key, shape, scale, limit, split=(), kind=jnp.bfloat16):
    result = jax.random.normal(own_key, shape, jnp.float32) * scale
    if len(split) > 0:
        result = shard_levels(own_key, shape, split, -0.22, 0.18) * result
    return jnp.clip(result, min=-limit, max=limit).astype(kind)


def setup_inputs(seed: int = 0) -> dict:
    key_of = jax.random.split(jax.random.key(seed), 5)
    return {
        "correlators": normal_values(key_of[0], (TW, NX, NY, NZ, 2 * CH), 1.0, 6.0, ((1, 4), (2, 4), (3, 2))),
        "momenta": set_ends(jax.random.randint(key_of[1], (MOM, 3), 0 - min(min(NX, NY), NZ) // 2, min(min(NX, NY), NZ) // 2), jax.random.fold_in(key_of[1], 1), 0 - min(min(NX, NY), NZ) // 2, (min(min(NX, NY), NZ) // 2) - 1).astype(jnp.int32),
        "source_channel": set_ends(jax.random.randint(key_of[2], (CH,), 0, CH), jax.random.fold_in(key_of[2], 1), 0, CH - 1).astype(jnp.int32),
        "phase_code": set_ends(jax.random.randint(key_of[3], (CH,), 0, 4), jax.random.fold_in(key_of[3], 1), 0, 3).astype(jnp.int32),
    }


def axis_fraction(values, coords, extent):
    return jnp.mod(values[:, None] * coords[None, :], extent).astype(jnp.float32) / extent

def phase_table(momenta, coord_x, coord_y, coord_z, size_x, size_y, size_z):
    frac_x = axis_fraction(momenta[:, 0], coord_x, size_x)
    frac_y = axis_fraction(momenta[:, 1], coord_y, size_y)
    frac_z = axis_fraction(momenta[:, 2], coord_z, size_z)
    summed = frac_x[:, :, None, None] + frac_y[:, None, :, None]
    summed = summed + frac_z[:, None, None, :]
    angles = (summed * (2.0 * math.pi)).reshape(momenta.shape[0], -1)
    return jnp.concatenate([jnp.cos(angles), jnp.sin(angles)], axis=0).astype(jnp.bfloat16)

def channel_signs(phase_code):
    real_sign = jnp.where(phase_code == 0, 1.0, jnp.where(phase_code == 2, -1.0, 0.0)).astype(jnp.float32)
    imag_sign = jnp.where(phase_code == 1, 1.0, jnp.where(phase_code == 3, -1.0, 0.0)).astype(jnp.float32)
    return (real_sign, imag_sign)

def reference(correlators, momenta, source_channel, phase_code):
    channels = correlators.shape[-1] // 2
    moment_count = momenta.shape[0]
    phases = phase_table(momenta, jnp.arange(NX, dtype=jnp.int32), jnp.arange(NY, dtype=jnp.int32), jnp.arange(NZ, dtype=jnp.int32), NX, NY, NZ).astype(jnp.float32)
    real_sign, imag_sign = channel_signs(phase_code)
    norm_factor = 1.0 / math.sqrt(NX * NY * NZ)

    def project(one_slice):
        values = one_slice.reshape(-1, 2 * channels).astype(jnp.float32)
        real_src = jnp.take(values[:, :channels], source_channel, axis=1)
        imag_src = jnp.take(values[:, channels:], source_channel, axis=1)
        real_mix = real_sign[None, :] * real_src - imag_sign[None, :] * imag_src
        imag_mix = imag_sign[None, :] * real_src + real_sign[None, :] * imag_src
        mixed = jnp.concatenate([real_mix, imag_mix], axis=1).astype(jnp.bfloat16)
        mixed = lax.optimization_barrier(mixed).astype(jnp.float32)
        product = jnp.dot(phases, mixed, preferred_element_type=jnp.float32)
        cos_part = product[:moment_count]
        sin_part = product[moment_count:]
        real_out = cos_part[:, :channels] + sin_part[:, channels:]
        imag_out = cos_part[:, channels:] - sin_part[:, :channels]
        return jnp.concatenate([real_out, imag_out], axis=1) * norm_factor
    return lax.map(project, correlators)
```

```python
import functools
import math

import jax
import jax.numpy as jnp
from jax import lax
from jax.experimental import pallas as pl
from jax.experimental.pallas import tpu as pltpu
from jax.sharding import PartitionSpec as P

LANES = 128
SUBLANES = 8
HALVES = 2


def round_up(value, unit):
    return (value + unit - 1) // unit * unit


def kernel(dims, corr, momenta, source, code, out, *scratch):
    (nx, ny, nz, na, nb, tpo, chunks, cells, sites, width, mom, cb, cbp, norm) = dims
    (raw, table, phases, part, got_a, send_b1, got_b1, send_b2, got_b2, send_c, got_c,
     load_sem, sa, ra, sb1, rb1, sb2, rb2, sc, rc) = scratch
    cells_x, cells_y, cells_z = cells
    lanes = table.shape[1]
    channels = width // 2
    rows = ny * cbp
    me_x, me_y, me_z = lax.axis_index("gx"), lax.axis_index("gy"), lax.axis_index("gz")
    me_a, me_b = me_x // nb, lax.rem(me_x, nb)

    loads = {}
    for j in range(chunks):
        for g in range(nx):
            at = pl.ds(g * tpo + j * HALVES, HALVES)
            loads[j, g] = pltpu.make_async_copy(corr.at[at], raw.at[at], load_sem.at[j, g])
            loads[j, g].start()

    def at_z(o):
        return {"gz": lax.rem(me_z + o, nz)}

    def at_a(o):
        return {"gx": lax.rem(me_a + o, na) * nb + me_b}

    def at_b(o):
        return {"gx": me_a * nb + lax.rem(me_b + o, nb)}

    def at_y(o):
        return {"gy": lax.rem(me_y + o, ny)}

    partners = [at_z(o) for o in range(1, nz)] + [at_a(o) for o in range(1, na)]
    partners += [at_b(o) for o in range(1, nb)] + [at_y(o) for o in range(1, ny)]
    barrier = pltpu.get_barrier_semaphore()
    for where in partners:
        pl.semaphore_signal(barrier, inc=1, device_id=where, device_id_type=pl.DeviceIdType.MESH)

    table[...] = jnp.zeros_like(table)
    table[0:3, 0:mom] = momenta[...]
    ks = table[...].astype(jnp.float32)

    def axis_table(axis, count, offset, extent):
        coord = lax.broadcasted_iota(jnp.int32, (count, lanes), 0) + offset
        turns = ks[axis:axis + 1, :] * coord.astype(jnp.float32) * (1.0 / extent)
        angle = (turns - jnp.floor(turns)) * (2.0 * math.pi)
        return jnp.cos(angle), jnp.sin(angle)

    cx, sx = axis_table(0, cells_x, me_x * cells_x, cells_x * nx)
    cy, sy = axis_table(1, cells_y, me_y * cells_y, cells_y * ny)
    cz, sz = axis_table(2, cells_z, me_z * cells_z, cells_z * nz)
    for x in range(cells_x):
        cxx, sxx = cx[x:x + 1], sx[x:x + 1]
        cxy, sxy = cxx * cy - sxx * sy, sxx * cy + cxx * sy
        for y in range(cells_y):
            c1, s1 = cxy[y:y + 1], sxy[y:y + 1]
            at = (x * cells_y + y) * cells_z
            phases[at:at + cells_z, 0:lanes] = (c1 * cz - s1 * sz).astype(phases.dtype)
            phases[at:at + cells_z, lanes:] = (s1 * cz + c1 * sz).astype(phases.dtype)

    total_rows = nz * rows
    row = lax.broadcasted_iota(jnp.int32, (total_rows, channels), 0)
    lane = lax.broadcasted_iota(jnp.int32, (total_rows, channels), 1)
    row_z, row_y, row_r = row // rows, (row % rows) // cbp, row % cbp
    channel = (row_y * nz + row_z) * cb + row_r
    is_imag = channel >= channels
    picked = lane == jnp.where(is_imag, channel - channels, channel)
    src = jnp.sum(jnp.where(picked, source[...].astype(jnp.float32), 0.0), axis=1, keepdims=True)
    cod = jnp.sum(jnp.where(picked, code[...].astype(jnp.float32), 0.0), axis=1, keepdims=True)
    row = lax.broadcasted_iota(jnp.int32, (total_rows, width), 0)
    k = lax.broadcasted_iota(jnp.int32, (total_rows, width), 1)
    row_z, row_y, row_r = row // rows, (row % rows) // cbp, row % cbp
    is_imag = (row_y * nz + row_z) * cb + row_r >= channels
    from_imag = k >= channels
    quarter = cod + jnp.where(from_imag, 1.0, 0.0) + jnp.where(is_imag, 3.0, 0.0)
    sign = jnp.where((quarter == 0.0) | (quarter == 4.0), 1.0, 0.0)
    sign = sign - jnp.where((quarter == 2.0) | (quarter == 6.0), 1.0, 0.0)
    hit = (jnp.where(from_imag, k - channels, k).astype(jnp.float32) == src) & (row_r < cb)
    mixing = jnp.where(hit, sign, 0.0).astype(jnp.bfloat16)

    def compute(j):
        for g in range(nx):
            loads[j, g].wait()
            first = g * tpo + j * HALVES
            block = raw[first:first + HALVES].reshape(HALVES * sites, width)
            mixed = lax.dot_general(
                mixing, block, (((1,), (1,)), ((), ())), preferred_element_type=jnp.float32
            ).astype(jnp.bfloat16)
            stacked = jnp.concatenate(
                [mixed[:, u * sites:(u + 1) * sites] for u in range(HALVES)], axis=0
            )
            product = jnp.dot(stacked, phases[...], preferred_element_type=jnp.float32)
            for u in range(HALVES):
                order = g // nb, g % nb
                place = order[1] * na + order[0] if u == 0 else g
                for z in range(nz):
                    at = u * total_rows + z * rows
                    mid = at + rows // 2
                    re, im = product[at:mid], product[mid:at + rows]
                    part[j, z, u, place, 0:rows // 2] = re[:, :lanes] + im[:, lanes:]
                    part[j, z, u, place, rows // 2:] = im[:, :lanes] - re[:, lanes:]

    def remote(src_ref, dst_ref, send, recv, where):
        return pltpu.make_async_remote_copy(
            src_ref=src_ref, dst_ref=dst_ref, send_sem=send, recv_sem=recv,
            device_id=where, device_id_type=pl.DeviceIdType.MESH,
        )

    sent = []
    a_copies, b1_copies, b2_copies, c_copies = {}, {}, {}, {}
    lead = (nb, na)
    trail = (na, nb)
    me_lead = (me_b, me_a)
    me_trail = (me_a, me_b)
    at_lead = (at_b, at_a)
    at_trail = (at_a, at_b)

    def send_stage_a(j):
        for o in range(1, nz):
            copy = remote(part.at[j, lax.rem(me_z + o, nz)], got_a.at[j, o - 1],
                          sa.at[j, o - 1], ra.at[j, o - 1], at_z(o))
            copy.start()
            a_copies.setdefault(j, []).append(copy)
            sent.append(copy)

    def sum_a(j, u, place):
        value = part[j, me_z, u, place]
        for o in range(nz - 1):
            value = value + got_a[j, o, u, place]
        return value

    def stage_b1(j):
        for copy in a_copies[j]:
            copy.wait_recv()
        for u in range(HALVES):
            for o in range(1, lead[u]):
                target = lax.rem(me_lead[u] + o, lead[u])
                for i in range(trail[u]):
                    send_b1[u][j, o - 1, i] = sum_a(j, u, target * trail[u] + i)
                copy = remote(send_b1[u].at[j, o - 1], got_b1[u].at[j, o - 1],
                              sb1[u].at[j, o - 1], rb1[u].at[j, o - 1], at_lead[u](o))
                copy.start()
                b1_copies.setdefault((j, u), []).append(copy)
                sent.append(copy)

    def sum_b1(j, u, i):
        value = sum_a(j, u, me_lead[u] * trail[u] + i)
        for o in range(lead[u] - 1):
            value = value + got_b1[u][j, o, i]
        return value

    def stage_b2(j):
        for u in range(HALVES):
            for copy in b1_copies.get((j, u), []):
                copy.wait_recv()
            for o in range(1, trail[u]):
                target = lax.rem(me_trail[u] + o, trail[u])
                send_b2[u][j, o - 1] = sum_b1(j, u, target)
                copy = remote(send_b2[u].at[j, o - 1], got_b2[u].at[j, o - 1],
                              sb2[u].at[j, o - 1], rb2[u].at[j, o - 1], at_trail[u](o))
                copy.start()
                b2_copies.setdefault((j, u), []).append(copy)
                sent.append(copy)

    def stage_c(j):
        for u in range(HALVES):
            for copy in b2_copies.get((j, u), []):
                copy.wait_recv()
            value = sum_b1(j, u, me_trail[u])
            for o in range(trail[u] - 1):
                value = value + got_b2[u][j, o]
            for y in range(ny):
                send_c[j, y, u] = value[y * cbp:(y + 1) * cbp]
        for o in range(1, ny):
            copy = remote(send_c.at[j, lax.rem(me_y + o, ny)], got_c.at[j, o - 1],
                          sc.at[j, o - 1], rc.at[j, o - 1], at_y(o))
            copy.start()
            c_copies.setdefault(j, []).append(copy)
            sent.append(copy)

    def finish(j):
        for copy in c_copies.get(j, []):
            copy.wait_recv()
        for u in range(HALVES):
            value = send_c[j, me_y, u]
            for o in range(ny - 1):
                value = value + got_c[j, o, u]
            out[j * HALVES + u] = (value * norm)[:, :mom]

    compute(0)
    pl.semaphore_wait(barrier, len(partners))
    send_stage_a(0)
    stages = (stage_b1, stage_b2, stage_c, finish)
    for step in range(1, chunks + len(stages)):
        if step < chunks:
            compute(step)
            send_stage_a(step)
        for depth, stage in enumerate(stages):
            j = step - 1 - depth
            if 0 <= j < chunks:
                stage(j)
    for copy in sent:
        copy.wait_send()


def local(axis_sizes, correlators, momenta, source_channel, phase_code):
    nx, ny, nz = axis_sizes
    window, cells_x, cells_y, cells_z, width = correlators.shape
    mom = momenta.shape[0]
    nb = 2 if nx % 2 == 0 else 1
    na = nx // nb
    tpo = window // nx
    chunks = tpo // HALVES
    cb = width // (ny * nz)
    cbp = round_up(cb, SUBLANES)
    rows = ny * cbp
    sites = cells_x * cells_y * cells_z
    lanes = round_up(mom, LANES)
    norm = 1.0 / math.sqrt(sites * nx * ny * nz)
    dims = (nx, ny, nz, na, nb, tpo, chunks, (cells_x, cells_y, cells_z), sites, width, mom, cb, cbp, norm)

    def buffer(*shape):
        return pltpu.VMEM(shape, jnp.float32)

    def sems(*shape):
        return pltpu.SemaphoreType.DMA(shape)

    def less(count):
        return max(count - 1, 1)

    lead, trail = (nb, na), (na, nb)
    scratch = [
        pltpu.VMEM((window, sites, width), correlators.dtype),
        pltpu.VMEM((SUBLANES, lanes), jnp.int32),
        pltpu.VMEM((sites, 2 * lanes), jnp.bfloat16),
        buffer(chunks, nz, HALVES, nx, rows, lanes),
        buffer(chunks, less(nz), HALVES, nx, rows, lanes),
        [buffer(chunks, less(lead[u]), trail[u], rows, lanes) for u in range(HALVES)],
        [buffer(chunks, less(lead[u]), trail[u], rows, lanes) for u in range(HALVES)],
        [buffer(chunks, less(trail[u]), rows, lanes) for u in range(HALVES)],
        [buffer(chunks, less(trail[u]), rows, lanes) for u in range(HALVES)],
        buffer(chunks, ny, HALVES, cbp, lanes),
        buffer(chunks, less(ny), HALVES, cbp, lanes),
        sems(chunks, nx),
        sems(chunks, less(nz)),
        sems(chunks, less(nz)),
        [sems(chunks, less(lead[u])) for u in range(HALVES)],
        [sems(chunks, less(lead[u])) for u in range(HALVES)],
        [sems(chunks, less(trail[u])) for u in range(HALVES)],
        [sems(chunks, less(trail[u])) for u in range(HALVES)],
        sems(chunks, less(ny)),
        sems(chunks, less(ny)),
    ]
    vmem = pl.BlockSpec(memory_space=pltpu.VMEM)
    result = pl.pallas_call(
        functools.partial(kernel, dims),
        out_shape=jax.ShapeDtypeStruct((tpo, cbp, mom), jnp.float32),
        in_specs=[pl.BlockSpec(memory_space=pl.ANY), vmem, vmem, vmem],
        out_specs=vmem,
        scratch_shapes=scratch,
        compiler_params=pltpu.CompilerParams(
            collective_id=0, has_side_effects=True, vmem_limit_bytes=48 * 1024 * 1024
        ),
        name="project",
    )(
        correlators.reshape(window, sites, width),
        momenta.T,
        source_channel.reshape(1, -1),
        phase_code.reshape(1, -1),
    )
    return jnp.swapaxes(result[:, :cb], 1, 2)


def solution(mesh):
    axis_sizes = tuple(mesh.shape[name] for name in ("gx", "gy", "gz"))
    in_specs = (P(None, "gx", "gy", "gz", None), P(), P(), P())
    out_specs = P("gx", None, ("gy", "gz"))
    return jax.shard_map(
        functools.partial(local, axis_sizes),
        mesh=mesh, in_specs=in_specs, out_specs=out_specs, check_vma=False,
    )
```

```python
import functools
import math

import jax
import jax.numpy as jnp
from jax import lax
from jax.experimental import pallas as pl
from jax.experimental.pallas import tpu as pltpu
from jax.sharding import PartitionSpec as P

LANES = 128
SUBLANES = 8
HALVES = 2


def round_up(value, unit):
    return (value + unit - 1) // unit * unit


def kernel(dims, corr, small, out, *scratch):
    (nx, ny, nz, na, nb, tpo, chunks, cells, sites, width, mom, cb, cbp, norm) = dims
    (raw, phases, part, got_a, send_b1, got_b1, send_b2, got_b2, send_c, got_c,
     load_sem, sa, ra, sb1, rb1, sb2, rb2, sc, rc) = scratch
    cells_x, cells_y, cells_z = cells
    lanes = phases.shape[1] // 2
    channels = width // 2
    rows = ny * cbp
    me_x, me_y, me_z = lax.axis_index("gx"), lax.axis_index("gy"), lax.axis_index("gz")
    me_a, me_b = me_x // nb, lax.rem(me_x, nb)

    loads = {}
    for j in range(chunks):
        for g in range(nx):
            at = pl.ds(g * tpo + j * HALVES, HALVES)
            loads[j, g] = pltpu.make_async_copy(corr.at[at], raw.at[at], load_sem.at[j, g])
            loads[j, g].start()

    def at_z(o):
        return {"gz": lax.rem(me_z + o, nz)}

    def at_a(o):
        return {"gx": lax.rem(me_a + o, na) * nb + me_b}

    def at_b(o):
        return {"gx": me_a * nb + lax.rem(me_b + o, nb)}

    def at_y(o):
        return {"gy": lax.rem(me_y + o, ny)}

    partners = [at_z(o) for o in range(1, nz)] + [at_a(o) for o in range(1, na)]
    partners += [at_b(o) for o in range(1, nb)] + [at_y(o) for o in range(1, ny)]
    barrier = pltpu.get_barrier_semaphore()
    for where in partners:
        pl.semaphore_signal(barrier, inc=1, device_id=where, device_id_type=pl.DeviceIdType.MESH)

    ks = small[0:3, 0:lanes].astype(jnp.float32)
    source, code = small[3:4, 0:width // 2], small[4:5, 0:width // 2]

    def axis_table(axis, count, offset, extent):
        coord = lax.broadcasted_iota(jnp.int32, (count, lanes), 0) + offset
        turns = ks[axis:axis + 1, :] * coord.astype(jnp.float32) * (1.0 / extent)
        angle = (turns - jnp.floor(turns)) * (2.0 * math.pi)
        return jnp.cos(angle), jnp.sin(angle)

    cx, sx = axis_table(0, cells_x, me_x * cells_x, cells_x * nx)
    cy, sy = axis_table(1, cells_y, me_y * cells_y, cells_y * ny)
    cz, sz = axis_table(2, cells_z, me_z * cells_z, cells_z * nz)
    for x in range(cells_x):
        cxx, sxx = cx[x:x + 1], sx[x:x + 1]
        cxy, sxy = cxx * cy - sxx * sy, sxx * cy + cxx * sy
        for y in range(cells_y):
            c1, s1 = cxy[y:y + 1], sxy[y:y + 1]
            at = (x * cells_y + y) * cells_z
            phases[at:at + cells_z, 0:lanes] = (c1 * cz - s1 * sz).astype(phases.dtype)
            phases[at:at + cells_z, lanes:] = (s1 * cz + c1 * sz).astype(phases.dtype)

    total_rows = nz * rows
    row = lax.broadcasted_iota(jnp.int32, (total_rows, channels), 0)
    lane = lax.broadcasted_iota(jnp.int32, (total_rows, channels), 1)
    row_z, row_y, row_r = row // rows, (row % rows) // cbp, row % cbp
    channel = (row_y * nz + row_z) * cb + row_r
    is_imag = channel >= channels
    picked = lane == jnp.where(is_imag, channel - channels, channel)
    src = jnp.sum(jnp.where(picked, source.astype(jnp.float32), 0.0), axis=1, keepdims=True)
    cod = jnp.sum(jnp.where(picked, code.astype(jnp.float32), 0.0), axis=1, keepdims=True)
    row = lax.broadcasted_iota(jnp.int32, (total_rows, width), 0)
    k = lax.broadcasted_iota(jnp.int32, (total_rows, width), 1)
    row_z, row_y, row_r = row // rows, (row % rows) // cbp, row % cbp
    is_imag = (row_y * nz + row_z) * cb + row_r >= channels
    from_imag = k >= channels
    quarter = cod + jnp.where(from_imag, 1.0, 0.0) + jnp.where(is_imag, 3.0, 0.0)
    sign = jnp.where((quarter == 0.0) | (quarter == 4.0), 1.0, 0.0)
    sign = sign - jnp.where((quarter == 2.0) | (quarter == 6.0), 1.0, 0.0)
    hit = (jnp.where(from_imag, k - channels, k).astype(jnp.float32) == src) & (row_r < cb)
    mixing = jnp.where(hit, sign, 0.0).astype(jnp.bfloat16)

    def compute(j):
        for g in range(nx):
            loads[j, g].wait()
            first = g * tpo + j * HALVES
            block = raw[first:first + HALVES].reshape(HALVES * sites, width)
            mixed = lax.dot_general(
                mixing, block, (((1,), (1,)), ((), ())), preferred_element_type=jnp.float32
            ).astype(jnp.bfloat16)
            stacked = jnp.concatenate(
                [mixed[:, u * sites:(u + 1) * sites] for u in range(HALVES)], axis=0
            )
            product = jnp.dot(stacked, phases[...], preferred_element_type=jnp.float32)
            for u in range(HALVES):
                order = g // nb, g % nb
                place = order[1] * na + order[0] if u == 0 else g
                for z in range(nz):
                    at = u * total_rows + z * rows
                    mid = at + rows // 2
                    re, im = product[at:mid], product[mid:at + rows]
                    part[j, z, u, place, 0:rows // 2] = re[:, :lanes] + im[:, lanes:]
                    part[j, z, u, place, rows // 2:] = im[:, :lanes] - re[:, lanes:]

    def remote(src_ref, dst_ref, send, recv, where):
        return pltpu.make_async_remote_copy(
            src_ref=src_ref, dst_ref=dst_ref, send_sem=send, recv_sem=recv,
            device_id=where, device_id_type=pl.DeviceIdType.MESH,
        )

    sent = []
    a_copies, b1_copies, b2_copies, c_copies = {}, {}, {}, {}
    lead = (nb, na)
    trail = (na, nb)
    me_lead = (me_b, me_a)
    me_trail = (me_a, me_b)
    at_lead = (at_b, at_a)
    at_trail = (at_a, at_b)

    def send_stage_a(j):
        for o in range(1, nz):
            copy = remote(part.at[j, lax.rem(me_z + o, nz)], got_a.at[j, o - 1],
                          sa.at[j, o - 1], ra.at[j, o - 1], at_z(o))
            copy.start()
            a_copies.setdefault(j, []).append(copy)
            sent.append(copy)

    def sum_a(j, u, place):
        value = part[j, me_z, u, place]
        for o in range(nz - 1):
            value = value + got_a[j, o, u, place]
        return value

    def stage_b1(j):
        for copy in a_copies[j]:
            copy.wait_recv()
        for u in range(HALVES):
            for o in range(1, lead[u]):
                target = lax.rem(me_lead[u] + o, lead[u])
                for i in range(trail[u]):
                    send_b1[u][j, o - 1, i] = sum_a(j, u, target * trail[u] + i)
                copy = remote(send_b1[u].at[j, o - 1], got_b1[u].at[j, o - 1],
                              sb1[u].at[j, o - 1], rb1[u].at[j, o - 1], at_lead[u](o))
                copy.start()
                b1_copies.setdefault((j, u), []).append(copy)
                sent.append(copy)

    def sum_b1(j, u, i):
        value = sum_a(j, u, me_lead[u] * trail[u] + i)
        for o in range(lead[u] - 1):
            value = value + got_b1[u][j, o, i]
        return value

    def stage_b2(j):
        for u in range(HALVES):
            for copy in b1_copies.get((j, u), []):
                copy.wait_recv()
            for o in range(1, trail[u]):
                target = lax.rem(me_trail[u] + o, trail[u])
                send_b2[u][j, o - 1] = sum_b1(j, u, target)
                copy = remote(send_b2[u].at[j, o - 1], got_b2[u].at[j, o - 1],
                              sb2[u].at[j, o - 1], rb2[u].at[j, o - 1], at_trail[u](o))
                copy.start()
                b2_copies.setdefault((j, u), []).append(copy)
                sent.append(copy)

    def stage_c(j):
        for u in range(HALVES):
            for copy in b2_copies.get((j, u), []):
                copy.wait_recv()
            value = sum_b1(j, u, me_trail[u])
            for o in range(trail[u] - 1):
                value = value + got_b2[u][j, o]
            for y in range(ny):
                send_c[j, y, u] = value[y * cbp:(y + 1) * cbp]
        for o in range(1, ny):
            copy = remote(send_c.at[j, lax.rem(me_y + o, ny)], got_c.at[j, o - 1],
                          sc.at[j, o - 1], rc.at[j, o - 1], at_y(o))
            copy.start()
            c_copies.setdefault(j, []).append(copy)
            sent.append(copy)

    def finish(j):
        for copy in c_copies.get(j, []):
            copy.wait_recv()
        for u in range(HALVES):
            value = send_c[j, me_y, u]
            for o in range(ny - 1):
                value = value + got_c[j, o, u]
            out[j * HALVES + u] = (value * norm)[:, :mom]

    compute(0)
    pl.semaphore_wait(barrier, len(partners))
    send_stage_a(0)
    stages = (stage_b1, stage_b2, stage_c, finish)
    for step in range(1, chunks + len(stages)):
        if step < chunks:
            compute(step)
            send_stage_a(step)
        for depth, stage in enumerate(stages):
            j = step - 1 - depth
            if 0 <= j < chunks:
                stage(j)
    for copy in sent:
        copy.wait_send()


def local(axis_sizes, correlators, momenta, source_channel, phase_code):
    nx, ny, nz = axis_sizes
    window, cells_x, cells_y, cells_z, width = correlators.shape
    mom = momenta.shape[0]
    nb = 2 if nx % 2 == 0 else 1
    na = nx // nb
    tpo = window // nx
    chunks = tpo // HALVES
    cb = width // (ny * nz)
    cbp = round_up(cb, SUBLANES)
    rows = ny * cbp
    sites = cells_x * cells_y * cells_z
    lanes = round_up(mom, LANES)
    norm = 1.0 / math.sqrt(sites * nx * ny * nz)
    dims = (nx, ny, nz, na, nb, tpo, chunks, (cells_x, cells_y, cells_z), sites, width, mom, cb, cbp, norm)

    small_lanes = max(lanes, round_up(width // 2, LANES))
    small = sum(
        jnp.pad(row, ((at, SUBLANES - at - row.shape[0]), (0, small_lanes - row.shape[1])))
        for at, row in ((0, momenta.T), (3, source_channel[None]), (4, phase_code[None]))
    )

    def buffer(*shape):
        return pltpu.VMEM(shape, jnp.float32)

    def sems(*shape):
        return pltpu.SemaphoreType.DMA(shape)

    def less(count):
        return max(count - 1, 1)

    lead, trail = (nb, na), (na, nb)
    scratch = [
        pltpu.VMEM((window, sites, width), correlators.dtype),
        pltpu.VMEM((sites, 2 * lanes), jnp.bfloat16),
        buffer(chunks, nz, HALVES, nx, rows, lanes),
        buffer(chunks, less(nz), HALVES, nx, rows, lanes),
        [buffer(chunks, less(lead[u]), trail[u], rows, lanes) for u in range(HALVES)],
        [buffer(chunks, less(lead[u]), trail[u], rows, lanes) for u in range(HALVES)],
        [buffer(chunks, less(trail[u]), rows, lanes) for u in range(HALVES)],
        [buffer(chunks, less(trail[u]), rows, lanes) for u in range(HALVES)],
        buffer(chunks, ny, HALVES, cbp, lanes),
        buffer(chunks, less(ny), HALVES, cbp, lanes),
        sems(chunks, nx),
        sems(chunks, less(nz)),
        sems(chunks, less(nz)),
        [sems(chunks, less(lead[u])) for u in range(HALVES)],
        [sems(chunks, less(lead[u])) for u in range(HALVES)],
        [sems(chunks, less(trail[u])) for u in range(HALVES)],
        [sems(chunks, less(trail[u])) for u in range(HALVES)],
        sems(chunks, less(ny)),
        sems(chunks, less(ny)),
    ]
    vmem, hbm = pl.BlockSpec(memory_space=pltpu.VMEM), pl.BlockSpec(memory_space=pltpu.HBM)
    result = pl.pallas_call(
        functools.partial(kernel, dims),
        out_shape=jax.ShapeDtypeStruct((tpo, cbp, mom), jnp.float32),
        in_specs=[hbm, vmem],
        out_specs=vmem,
        scratch_shapes=scratch,
        compiler_params=pltpu.CompilerParams(
            collective_id=0, has_side_effects=True, vmem_limit_bytes=52 * 1024 * 1024
        ),
        name="project",
    )(
        correlators.reshape(window, sites, width),
        small,
    )
    return jnp.swapaxes(result[:, :cb], 1, 2)


def solution(mesh):
    axis_sizes = tuple(mesh.shape[name] for name in ("gx", "gy", "gz"))
    in_specs = (P(None, "gx", "gy", "gz", None), P(), P(), P())
    out_specs = P("gx", None, ("gy", "gz"))
    return jax.shard_map(
        functools.partial(local, axis_sizes),
        mesh=mesh, in_specs=in_specs, out_specs=out_specs, check_vma=False,
    )
```

```python
import functools
import math

import jax
import jax.numpy as jnp
from jax import lax
from jax.experimental import pallas as pl
from jax.experimental.pallas import tpu as pltpu
from jax.sharding import PartitionSpec as P

LANES = 128
SUBLANES = 8
HALVES = 2
LAGS = (1, 4, 7, 10)
GROUP = 4


def round_up(value, unit):
    return (value + unit - 1) // unit * unit


def kernel(dims, corr, small, out, *scratch):
    (nx, ny, nz, na, nb, tpo, chunks, cells, sites, width, mom, cb, cbp, norm) = dims
    (raw, phases, part, got_a, send_b1, got_b1, send_b2, got_b2, send_c, got_c,
     load_sem, sa, ra, sb1, rb1, sb2, rb2, sc, rc) = scratch
    cells_x, cells_y, cells_z = cells
    lanes = phases.shape[1] // 2
    channels = width // 2
    rows = ny * cbp
    half_rows = rows // HALVES
    me_x, me_y, me_z = lax.axis_index("gx"), lax.axis_index("gy"), lax.axis_index("gz")
    me_a, me_b = me_x // nb, lax.rem(me_x, nb)

    def load(j, g):
        at = g * tpo + j
        return pltpu.make_async_copy(corr.at[at], raw.at[at], load_sem.at[j, g])

    @pl.loop(0, chunks)
    def _(j):
        for g in range(nx):
            load(j, g).start()

    def at_z(o):
        return {"gz": lax.rem(me_z + o, nz)}

    def at_a(o):
        return {"gx": lax.rem(me_a + o, na) * nb + me_b}

    def at_b(o):
        return {"gx": me_a * nb + lax.rem(me_b + o, nb)}

    def at_y(o):
        return {"gy": lax.rem(me_y + o, ny)}

    partners = [at_z(o) for o in range(1, nz)] + [at_a(o) for o in range(1, na)]
    partners += [at_b(o) for o in range(1, nb)] + [at_y(o) for o in range(1, ny)]
    barrier = pltpu.get_barrier_semaphore()
    for where in partners:
        pl.semaphore_signal(barrier, inc=1, device_id=where, device_id_type=pl.DeviceIdType.MESH)

    ks = small[0:3, 0:lanes].astype(jnp.float32)
    source, code = small[3:4, 0:width // 2], small[4:5, 0:width // 2]

    def axis_table(axis, count, offset, extent):
        coord = lax.broadcasted_iota(jnp.int32, (count, lanes), 0) + offset
        turns = ks[axis:axis + 1, :] * coord.astype(jnp.float32) * (1.0 / extent)
        angle = (turns - jnp.floor(turns)) * (2.0 * math.pi)
        return jnp.cos(angle), jnp.sin(angle)

    cx, sx = axis_table(0, cells_x, me_x * cells_x, cells_x * nx)
    cy, sy = axis_table(1, cells_y, me_y * cells_y, cells_y * ny)
    cz, sz = axis_table(2, cells_z, me_z * cells_z, cells_z * nz)
    for x in range(cells_x):
        cxx, sxx = cx[x:x + 1], sx[x:x + 1]
        cxy, sxy = cxx * cy - sxx * sy, sxx * cy + cxx * sy
        for y in range(cells_y):
            c1, s1 = cxy[y:y + 1], sxy[y:y + 1]
            at = (x * cells_y + y) * cells_z
            phases[at:at + cells_z, 0:lanes] = (c1 * cz - s1 * sz).astype(phases.dtype)
            phases[at:at + cells_z, lanes:] = (s1 * cz + c1 * sz).astype(phases.dtype)

    total_rows = nz * rows
    row = lax.broadcasted_iota(jnp.int32, (total_rows, channels), 0)
    lane = lax.broadcasted_iota(jnp.int32, (total_rows, channels), 1)
    row_z, row_y, row_r = row // rows, (row % rows) // cbp, row % cbp
    channel = (row_y * nz + row_z) * cb + row_r
    is_imag = channel >= channels
    picked = lane == jnp.where(is_imag, channel - channels, channel)
    src = jnp.sum(jnp.where(picked, source.astype(jnp.float32), 0.0), axis=1, keepdims=True)
    cod = jnp.sum(jnp.where(picked, code.astype(jnp.float32), 0.0), axis=1, keepdims=True)
    row = lax.broadcasted_iota(jnp.int32, (total_rows, width), 0)
    k = lax.broadcasted_iota(jnp.int32, (total_rows, width), 1)
    row_z, row_y, row_r = row // rows, (row % rows) // cbp, row % cbp
    is_imag = (row_y * nz + row_z) * cb + row_r >= channels
    from_imag = k >= channels
    quarter = cod + jnp.where(from_imag, 1.0, 0.0) + jnp.where(is_imag, 3.0, 0.0)
    sign = jnp.where((quarter == 0.0) | (quarter == 4.0), 1.0, 0.0)
    sign = sign - jnp.where((quarter == 2.0) | (quarter == 6.0), 1.0, 0.0)
    hit = (jnp.where(from_imag, k - channels, k).astype(jnp.float32) == src) & (row_r < cb)
    mixing = jnp.where(hit, sign, 0.0).astype(jnp.bfloat16)

    def compute(j):
        for first in range(0, nx, GROUP):
            owners = range(first, min(first + GROUP, nx))
            stacked = []
            for g in owners:
                load(j, g).wait()
                stacked.append(lax.dot_general(
                    mixing, raw[g * tpo + j], (((1,), (1,)), ((), ())),
                    preferred_element_type=jnp.float32,
                ).astype(jnp.bfloat16))
            stacked = jnp.concatenate(stacked, axis=0)
            product = jnp.dot(stacked, phases[...], preferred_element_type=jnp.float32)
            for g in owners:
                for z in range(nz):
                    at = (g - first) * total_rows + z * rows
                    mid = at + half_rows
                    re, im = product[at:mid], product[mid:at + rows]
                    place = (g % nb) * na + g // nb
                    part[j, z, 0, place] = re[:, :lanes] + im[:, lanes:]
                    part[j, z, 1, g] = im[:, :lanes] - re[:, lanes:]

    def remote(src_ref, dst_ref, send, recv, where):
        return pltpu.make_async_remote_copy(
            src_ref=src_ref, dst_ref=dst_ref, send_sem=send, recv_sem=recv,
            device_id=where, device_id_type=pl.DeviceIdType.MESH,
        )

    lead = (nb, na)
    trail = (na, nb)
    me_lead = (me_b, me_a)
    me_trail = (me_a, me_b)
    at_lead = (at_b, at_a)
    at_trail = (at_a, at_b)

    def a_copies(j):
        return [remote(part.at[j, lax.rem(me_z + o, nz)], got_a.at[j, o - 1],
                       sa.at[j, o - 1], ra.at[j, o - 1], at_z(o)) for o in range(1, nz)]

    def b1_copies(j, u):
        return [remote(send_b1[u].at[j, o - 1], got_b1[u].at[j, o - 1], sb1[u].at[j, o - 1],
                       rb1[u].at[j, o - 1], at_lead[u](o)) for o in range(1, lead[u])]

    def b2_copies(j, u):
        return [remote(send_b2[u].at[j, o - 1], got_b2[u].at[j, o - 1], sb2[u].at[j, o - 1],
                       rb2[u].at[j, o - 1], at_trail[u](o)) for o in range(1, trail[u])]

    def c_copies(j):
        return [remote(send_c.at[j, lax.rem(me_y + o, ny)], got_c.at[j, o - 1],
                       sc.at[j, o - 1], rc.at[j, o - 1], at_y(o)) for o in range(1, ny)]

    def send_stage_a(j):
        for copy in a_copies(j):
            copy.start()

    def sum_a(j, u, place):
        value = part[j, me_z, u, place]
        for o in range(nz - 1):
            value = value + got_a[j, o, u, place]
        return value

    def stage_b1(j):
        for copy in a_copies(j):
            copy.wait_recv()
        for u in range(HALVES):
            for o, copy in enumerate(b1_copies(j, u)):
                target = lax.rem(me_lead[u] + o + 1, lead[u])
                for i in range(trail[u]):
                    send_b1[u][j, o, i] = sum_a(j, u, target * trail[u] + i)
                copy.start()

    def sum_b1(j, u, i):
        value = sum_a(j, u, me_lead[u] * trail[u] + i)
        for o in range(lead[u] - 1):
            value = value + got_b1[u][j, o, i]
        return value

    def stage_b2(j):
        for u in range(HALVES):
            for copy in b1_copies(j, u):
                copy.wait_recv()
            for o, copy in enumerate(b2_copies(j, u)):
                send_b2[u][j, o] = sum_b1(j, u, lax.rem(me_trail[u] + o + 1, trail[u]))
                copy.start()

    def stage_c(j):
        for u in range(HALVES):
            for copy in b2_copies(j, u):
                copy.wait_recv()
            value = sum_b1(j, u, me_trail[u])
            for o in range(trail[u] - 1):
                value = value + got_b2[u][j, o]
            for y in range(ny // HALVES):
                send_c[j, u * (ny // HALVES) + y] = value[y * cbp:(y + 1) * cbp]
        for copy in c_copies(j):
            copy.start()

    def finish(j):
        for copy in c_copies(j):
            copy.wait_recv()
        value = send_c[j, me_y]
        for o in range(ny - 1):
            value = value + got_c[j, o]
        out[j] = (value * norm)[:, :mom]

    compute(0)
    pl.semaphore_wait(barrier, len(partners))
    send_stage_a(0)

    @pl.loop(1, chunks + LAGS[-1])
    def _(step):
        @pl.when(step < chunks)
        def _():
            compute(step)
            send_stage_a(step)

        for lag, stage in zip(LAGS, (stage_b1, stage_b2, stage_c, finish)):
            pl.when((step >= lag) & (step < chunks + lag))(functools.partial(stage, step - lag))

    @pl.loop(0, chunks)
    def _(j):
        for copy in a_copies(j) + c_copies(j):
            copy.wait_send()
        for u in range(HALVES):
            for copy in b1_copies(j, u) + b2_copies(j, u):
                copy.wait_send()


def local(axis_sizes, correlators, momenta, source_channel, phase_code):
    nx, ny, nz = axis_sizes
    window, cells_x, cells_y, cells_z, width = correlators.shape
    mom = momenta.shape[0]
    nb = 2 if nx % 2 == 0 else 1
    na = nx // nb
    tpo = window // nx
    chunks = tpo
    cb = width // (ny * nz)
    cbp = round_up(cb, SUBLANES)
    half_rows = ny * cbp // HALVES
    sites = cells_x * cells_y * cells_z
    lanes = round_up(mom, LANES)
    norm = 1.0 / math.sqrt(sites * nx * ny * nz)
    dims = (nx, ny, nz, na, nb, tpo, chunks, (cells_x, cells_y, cells_z), sites, width, mom, cb, cbp, norm)

    small_lanes = max(lanes, round_up(width // 2, LANES))
    small = sum(
        jnp.pad(row, ((at, SUBLANES - at - row.shape[0]), (0, small_lanes - row.shape[1])))
        for at, row in ((0, momenta.T), (3, source_channel[None]), (4, phase_code[None]))
    )

    def buffer(*shape):
        return pltpu.VMEM(shape, jnp.float32)

    def sems(*shape):
        return pltpu.SemaphoreType.DMA(shape)

    def less(count):
        return max(count - 1, 1)

    lead, trail = (nb, na), (na, nb)
    scratch = [
        pltpu.VMEM((window, sites, width), correlators.dtype),
        pltpu.VMEM((sites, 2 * lanes), jnp.bfloat16),
        buffer(chunks, nz, HALVES, nx, half_rows, lanes),
        buffer(chunks, less(nz), HALVES, nx, half_rows, lanes),
        [buffer(chunks, less(lead[u]), trail[u], half_rows, lanes) for u in range(HALVES)],
        [buffer(chunks, less(lead[u]), trail[u], half_rows, lanes) for u in range(HALVES)],
        [buffer(chunks, less(trail[u]), half_rows, lanes) for u in range(HALVES)],
        [buffer(chunks, less(trail[u]), half_rows, lanes) for u in range(HALVES)],
        buffer(chunks, ny, cbp, lanes),
        buffer(chunks, less(ny), cbp, lanes),
        sems(chunks, nx),
        sems(chunks, less(nz)),
        sems(chunks, less(nz)),
        [sems(chunks, less(lead[u])) for u in range(HALVES)],
        [sems(chunks, less(lead[u])) for u in range(HALVES)],
        [sems(chunks, less(trail[u])) for u in range(HALVES)],
        [sems(chunks, less(trail[u])) for u in range(HALVES)],
        sems(chunks, less(ny)),
        sems(chunks, less(ny)),
    ]
    vmem, hbm = pl.BlockSpec(memory_space=pltpu.VMEM), pl.BlockSpec(memory_space=pltpu.HBM)
    result = pl.pallas_call(
        functools.partial(kernel, dims),
        out_shape=jax.ShapeDtypeStruct((tpo, cbp, mom), jnp.float32),
        in_specs=[hbm, vmem],
        out_specs=vmem,
        scratch_shapes=scratch,
        compiler_params=pltpu.CompilerParams(
            collective_id=0, has_side_effects=True, vmem_limit_bytes=52 * 1024 * 1024
        ),
        name="project",
    )(
        correlators.reshape(window, sites, width),
        small,
    )
    return jnp.swapaxes(result[:, :cb], 1, 2)


def solution(mesh):
    axis_sizes = tuple(mesh.shape[name] for name in ("gx", "gy", "gz"))
    in_specs = (P(None, "gx", "gy", "gz", None), P(), P(), P())
    out_specs = P("gx", None, ("gy", "gz"))
    return jax.shard_map(
        functools.partial(local, axis_sizes),
        mesh=mesh, in_specs=in_specs, out_specs=out_specs, check_vma=False,
    )
```

```python
import functools
import math

import jax
import jax.numpy as jnp
from jax import lax
from jax.experimental import pallas as pl
from jax.experimental.pallas import tpu as pltpu
from jax.sharding import PartitionSpec as P

LANES = 128
SUBLANES = 8
HALVES = 2
LAGS = (1, 4, 8, 12)
GROUP = 4


def round_up(value, unit):
    return (value + unit - 1) // unit * unit


def kernel(dims, corr, small, out, *scratch):
    (nx, ny, nz, na, nb, tpo, chunks, cells, sites, width, mom, cb, cbp, norm) = dims
    (raw, phases, part, got_a, send_b1, got_b1, send_b2, got_b2, send_c, got_c,
     load_sem, sa, ra, sb1, rb1, sb2, rb2, sc, rc) = scratch
    cells_x, cells_y, cells_z = cells
    lanes = phases.shape[1] // 2
    channels = width // 2
    rows = ny * cbp
    half_rows = rows // HALVES
    me_x, me_y, me_z = lax.axis_index("gx"), lax.axis_index("gy"), lax.axis_index("gz")
    me_a, me_b = me_x // nb, lax.rem(me_x, nb)

    def load(j, g):
        at = g * tpo + j
        return pltpu.make_async_copy(corr.at[at], raw.at[at], load_sem.at[j, g])

    @pl.loop(0, chunks)
    def _(j):
        for g in range(nx):
            load(j, g).start()

    def at_z(o):
        return {"gz": lax.rem(me_z + o, nz)}

    def at_a(o):
        return {"gx": lax.rem(me_a + o, na) * nb + me_b}

    def at_b(o):
        return {"gx": me_a * nb + lax.rem(me_b + o, nb)}

    def at_y(o):
        return {"gy": lax.rem(me_y + o, ny)}

    partners = [at_z(o) for o in range(1, nz)] + [at_a(o) for o in range(1, na)]
    partners += [at_b(o) for o in range(1, nb)] + [at_y(o) for o in range(1, ny)]
    barrier = pltpu.get_barrier_semaphore()
    for where in partners:
        pl.semaphore_signal(barrier, inc=1, device_id=where, device_id_type=pl.DeviceIdType.MESH)

    ks = small[0:3, 0:lanes].astype(jnp.float32)
    source, code = small[3:4, 0:width // 2], small[4:5, 0:width // 2]

    def axis_table(axis, count, offset, extent):
        coord = lax.broadcasted_iota(jnp.int32, (count, lanes), 0) + offset
        turns = ks[axis:axis + 1, :] * coord.astype(jnp.float32) * (1.0 / extent)
        angle = (turns - jnp.floor(turns)) * (2.0 * math.pi)
        return jnp.cos(angle), jnp.sin(angle)

    cx, sx = axis_table(0, cells_x, me_x * cells_x, cells_x * nx)
    cy, sy = axis_table(1, cells_y, me_y * cells_y, cells_y * ny)
    cz, sz = axis_table(2, cells_z, me_z * cells_z, cells_z * nz)
    for x in range(cells_x):
        cxx, sxx = cx[x:x + 1], sx[x:x + 1]
        cxy, sxy = cxx * cy - sxx * sy, sxx * cy + cxx * sy
        for y in range(cells_y):
            c1, s1 = cxy[y:y + 1], sxy[y:y + 1]
            at = (x * cells_y + y) * cells_z
            phases[at:at + cells_z, 0:lanes] = (c1 * cz - s1 * sz).astype(phases.dtype)
            phases[at:at + cells_z, lanes:] = (s1 * cz + c1 * sz).astype(phases.dtype)

    total_rows = nz * rows
    row = lax.broadcasted_iota(jnp.int32, (total_rows, channels), 0)
    lane = lax.broadcasted_iota(jnp.int32, (total_rows, channels), 1)
    row_z, row_y, row_r = row // rows, (row % rows) // cbp, row % cbp
    channel = (row_y * nz + row_z) * cb + row_r
    is_imag = channel >= channels
    picked = lane == jnp.where(is_imag, channel - channels, channel)
    src = jnp.sum(jnp.where(picked, source.astype(jnp.float32), 0.0), axis=1, keepdims=True)
    cod = jnp.sum(jnp.where(picked, code.astype(jnp.float32), 0.0), axis=1, keepdims=True)
    row = lax.broadcasted_iota(jnp.int32, (total_rows, width), 0)
    k = lax.broadcasted_iota(jnp.int32, (total_rows, width), 1)
    row_z, row_y, row_r = row // rows, (row % rows) // cbp, row % cbp
    is_imag = (row_y * nz + row_z) * cb + row_r >= channels
    from_imag = k >= channels
    quarter = cod + jnp.where(from_imag, 1.0, 0.0) + jnp.where(is_imag, 3.0, 0.0)
    sign = jnp.where((quarter == 0.0) | (quarter == 4.0), 1.0, 0.0)
    sign = sign - jnp.where((quarter == 2.0) | (quarter == 6.0), 1.0, 0.0)
    hit = (jnp.where(from_imag, k - channels, k).astype(jnp.float32) == src) & (row_r < cb)
    mixing = jnp.where(hit, sign, 0.0).astype(jnp.bfloat16)

    def compute(j):
        for first in range(0, nx, GROUP):
            owners = range(first, min(first + GROUP, nx))
            stacked = []
            for g in owners:
                load(j, g).wait()
                stacked.append(lax.dot_general(
                    mixing, raw[g * tpo + j], (((1,), (1,)), ((), ())),
                    preferred_element_type=jnp.float32,
                ).astype(jnp.bfloat16))
            stacked = jnp.concatenate(stacked, axis=0)
            product = jnp.dot(stacked, phases[...], preferred_element_type=jnp.float32)
            for g in owners:
                for z in range(nz):
                    at = (g - first) * total_rows + z * rows
                    mid = at + half_rows
                    re, im = product[at:mid], product[mid:at + rows]
                    place = (g % nb) * na + g // nb
                    part[j, z, 0, place] = re[:, :lanes] + im[:, lanes:]
                    part[j, z, 1, g] = im[:, :lanes] - re[:, lanes:]

    def remote(src_ref, dst_ref, send, recv, where):
        return pltpu.make_async_remote_copy(
            src_ref=src_ref, dst_ref=dst_ref, send_sem=send, recv_sem=recv,
            device_id=where, device_id_type=pl.DeviceIdType.MESH,
        )

    lead = (nb, na)
    trail = (na, nb)
    me_lead = (me_b, me_a)
    me_trail = (me_a, me_b)
    at_lead = (at_b, at_a)
    at_trail = (at_a, at_b)

    def a_copies(j):
        return [remote(part.at[j, lax.rem(me_z + o, nz)], got_a.at[j, o - 1],
                       sa.at[j, o - 1], ra.at[j, o - 1], at_z(o)) for o in range(1, nz)]

    def b1_copies(j, u):
        return [remote(send_b1[u].at[j, o - 1], got_b1[u].at[j, o - 1], sb1[u].at[j, o - 1],
                       rb1[u].at[j, o - 1], at_lead[u](o)) for o in range(1, lead[u])]

    def b2_copies(j, u):
        return [remote(send_b2[u].at[j, o - 1], got_b2[u].at[j, o - 1], sb2[u].at[j, o - 1],
                       rb2[u].at[j, o - 1], at_trail[u](o)) for o in range(1, trail[u])]

    def c_copies(j):
        return [remote(send_c.at[j, lax.rem(me_y + o, ny)], got_c.at[j, o - 1],
                       sc.at[j, o - 1], rc.at[j, o - 1], at_y(o)) for o in range(1, ny)]

    def send_stage_a(j):
        for copy in a_copies(j):
            copy.start()

    def sum_a(j, u, place):
        value = part[j, me_z, u, place]
        for o in range(nz - 1):
            value = value + got_a[j, o, u, place]
        return value

    def stage_b1(j):
        for copy in a_copies(j):
            copy.wait_recv()
        for u in range(HALVES):
            for o, copy in enumerate(b1_copies(j, u)):
                target = lax.rem(me_lead[u] + o + 1, lead[u])
                for i in range(trail[u]):
                    send_b1[u][j, o, i] = sum_a(j, u, target * trail[u] + i)
                copy.start()

    def sum_b1(j, u, i):
        value = sum_a(j, u, me_lead[u] * trail[u] + i)
        for o in range(lead[u] - 1):
            value = value + got_b1[u][j, o, i]
        return value

    def stage_b2(j):
        for u in range(HALVES):
            for copy in b1_copies(j, u):
                copy.wait_recv()
            for o, copy in enumerate(b2_copies(j, u)):
                send_b2[u][j, o] = sum_b1(j, u, lax.rem(me_trail[u] + o + 1, trail[u]))
                copy.start()

    def stage_c(j):
        for u in range(HALVES):
            for copy in b2_copies(j, u):
                copy.wait_recv()
            value = sum_b1(j, u, me_trail[u])
            for o in range(trail[u] - 1):
                value = value + got_b2[u][j, o]
            for y in range(ny // HALVES):
                send_c[j, u * (ny // HALVES) + y] = value[y * cbp:(y + 1) * cbp]
        for copy in c_copies(j):
            copy.start()

    def finish(j):
        for copy in c_copies(j):
            copy.wait_recv()
        value = send_c[j, me_y]
        for o in range(ny - 1):
            value = value + got_c[j, o]
        out[j] = (value * norm)[:, :mom]

    compute(0)
    pl.semaphore_wait(barrier, len(partners))
    send_stage_a(0)

    @pl.loop(1, chunks + LAGS[-1])
    def _(step):
        @pl.when(step < chunks)
        def _():
            compute(step)
            send_stage_a(step)

        for lag, stage in zip(LAGS, (stage_b1, stage_b2, stage_c, finish)):
            pl.when((step >= lag) & (step < chunks + lag))(functools.partial(stage, step - lag))

    @pl.loop(0, chunks)
    def _(j):
        for copy in a_copies(j) + c_copies(j):
            copy.wait_send()
        for u in range(HALVES):
            for copy in b1_copies(j, u) + b2_copies(j, u):
                copy.wait_send()


def local(axis_sizes, correlators, momenta, source_channel, phase_code):
    nx, ny, nz = axis_sizes
    window, cells_x, cells_y, cells_z, width = correlators.shape
    mom = momenta.shape[0]
    nb = 2 if nx % 2 == 0 else 1
    na = nx // nb
    tpo = window // nx
    chunks = tpo
    cb = width // (ny * nz)
    cbp = round_up(cb, SUBLANES)
    half_rows = ny * cbp // HALVES
    sites = cells_x * cells_y * cells_z
    lanes = round_up(mom, LANES)
    norm = 1.0 / math.sqrt(sites * nx * ny * nz)
    dims = (nx, ny, nz, na, nb, tpo, chunks, (cells_x, cells_y, cells_z), sites, width, mom, cb, cbp, norm)

    small_lanes = max(lanes, round_up(width // 2, LANES))
    small = sum(
        jnp.pad(row, ((at, SUBLANES - at - row.shape[0]), (0, small_lanes - row.shape[1])))
        for at, row in ((0, momenta.T), (3, source_channel[None]), (4, phase_code[None]))
    )

    def buffer(*shape):
        return pltpu.VMEM(shape, jnp.float32)

    def sems(*shape):
        return pltpu.SemaphoreType.DMA(shape)

    def less(count):
        return max(count - 1, 1)

    lead, trail = (nb, na), (na, nb)
    scratch = [
        pltpu.VMEM((window, sites, width), correlators.dtype),
        pltpu.VMEM((sites, 2 * lanes), jnp.bfloat16),
        buffer(chunks, nz, HALVES, nx, half_rows, lanes),
        buffer(chunks, less(nz), HALVES, nx, half_rows, lanes),
        [buffer(chunks, less(lead[u]), trail[u], half_rows, lanes) for u in range(HALVES)],
        [buffer(chunks, less(lead[u]), trail[u], half_rows, lanes) for u in range(HALVES)],
        [buffer(chunks, less(trail[u]), half_rows, lanes) for u in range(HALVES)],
        [buffer(chunks, less(trail[u]), half_rows, lanes) for u in range(HALVES)],
        buffer(chunks, ny, cbp, lanes),
        buffer(chunks, less(ny), cbp, lanes),
        sems(chunks, nx),
        sems(chunks, less(nz)),
        sems(chunks, less(nz)),
        [sems(chunks, less(lead[u])) for u in range(HALVES)],
        [sems(chunks, less(lead[u])) for u in range(HALVES)],
        [sems(chunks, less(trail[u])) for u in range(HALVES)],
        [sems(chunks, less(trail[u])) for u in range(HALVES)],
        sems(chunks, less(ny)),
        sems(chunks, less(ny)),
    ]
    vmem, hbm = pl.BlockSpec(memory_space=pltpu.VMEM), pl.BlockSpec(memory_space=pltpu.HBM)
    result = pl.pallas_call(
        functools.partial(kernel, dims),
        out_shape=jax.ShapeDtypeStruct((tpo, cbp, mom), jnp.float32),
        in_specs=[hbm, vmem],
        out_specs=vmem,
        scratch_shapes=scratch,
        compiler_params=pltpu.CompilerParams(
            collective_id=0, has_side_effects=True, vmem_limit_bytes=52 * 1024 * 1024
        ),
        name="project",
    )(
        correlators.reshape(window, sites, width),
        small,
    )
    return jnp.swapaxes(result[:, :cb], 1, 2)


def solution(mesh):
    axis_sizes = tuple(mesh.shape[name] for name in ("gx", "gy", "gz"))
    in_specs = (P(None, "gx", "gy", "gz", None), P(), P(), P())
    out_specs = P("gx", None, ("gy", "gz"))
    return jax.shard_map(
        functools.partial(local, axis_sizes),
        mesh=mesh, in_specs=in_specs, out_specs=out_specs, check_vma=False,
    )
```
